256 devices in a mesh: band: 8 (over y, core), col: 32 (over z, x).
Axes of the slice: x: 4, y: 4, z: 8, core: 2. Of those that a mesh axis runs over, the one named last changes fastest.
Arguments:
- source: bfloat16 [6, 4194304], P(None, ('band', 'col')), may hold values from -6 to 6
- weights: bfloat16 [65536, 128, 128], P(('band', 'col')), may hold values from -0.5 to 0.5
- source_block: int32 [65536], P(('band', 'col')), may hold values from 0 to 127
- owner_device: int32 [65536, 1], P(('band', 'col')), may hold values from 0 to 255, as said below
- target_tile: int32 [65536], P(('band', 'col')), may hold values from 0 to 112, as said below
- cutoff: int32 [512], P(('band', 'col')), may hold values from 1 to 511
Outputs:
- remapped: float32 [6, 512, 7200], P(None, 'band', 'col')
- filtered: float32 [6, 512, 7200], P(None, 'band', 'col')
The draws below stay inside these ranges and needn't reach their ends.
Inputs may be any that keep to these rules, and one draw needn't show every extreme that they name: `owner_device`: owners are numbered band index times 32 plus col index. A device's blocks go only to owners in its own band or in the bands next to it. Among the 256 blocks of one device at most 6 share an owner; in every device exactly 6 do for some owner of its own band, and exactly 6 for some owner of each band next to its own; every device sends at least 4 blocks to each owner of its own band. `target_tile`: every tile of every owner receives at least one block.
All inputs are finite; a program needn't handle non-finite values.
Results may differ from the reference program's by a relative error of at most 0.0003.
Values sent between devices are 32-bit elements; how exact they have to be, the bound alone decides.
No kernel may reach another device: no remote copies, remote signals or barrier semaphores. Data moves between devices by JAX's collectives and lax.ppermute only.
A program may use at most 64 MiB of HBM per device.

```python
import jax
import jax.numpy as jnp
from jax import lax

NLON = 7200
BLK = 128
LEV = 6
KW = 512
NB = 256
SB = 128
LATB = 64
NLAT = 512
LON_DEV = 225
TILES_DEV = 113
REG = 4
CAP = 6
NBLOCKS = 65536
NSRC = 4194304
N_BAND = 8
N_COL = 32
DEVICES = 256


def remap_layout(key):
    slot_total = 3 * N_COL * CAP
    slots = jnp.arange(slot_total, dtype=jnp.int32)
    offset = slots // (N_COL * CAP)
    owner_col = slots // CAP % N_COL
    within = slots % CAP
    shifts = jax.random.randint(jax.random.fold_in(key, 11), (DEVICES,), 0, TILES_DEV).astype(jnp.int32)

    def one_device(device):
        device_key = jax.random.fold_in(jax.random.fold_in(key, 17), device)
        band = device // N_COL
        column = device % N_COL
        owner_band = band + offset - 1
        valid = (owner_band >= 0) & (owner_band < N_BAND)
        regular = (offset == 1) & (within < REG)
        candidate = valid & ((offset != 1) | (within >= REG))
        forced_cols = jax.random.randint(jax.random.fold_in(device_key, 1), (3,), 0, N_COL).astype(jnp.int32)
        forced = candidate & (owner_col == forced_cols[offset])
        ranking = jax.random.permutation(jax.random.fold_in(device_key, 2), slot_total).astype(jnp.int32)
        score = jnp.where(regular, 0, jnp.where(forced, 1, jnp.where(candidate, 2 + ranking, 4 * slot_total + 4)))
        chosen = jnp.argsort(score, stable=True)[:NB].astype(jnp.int32)
        mixing = jax.random.permutation(jax.random.fold_in(device_key, 3), NB).astype(jnp.int32)
        chosen = chosen[mixing]
        owners = (owner_band[chosen] * N_COL + owner_col[chosen]).astype(jnp.int32)
        random_tile = jax.random.randint(jax.random.fold_in(device_key, 4), (NB,), 0, TILES_DEV).astype(jnp.int32)
        regular_tile = (column * REG + within[chosen] + shifts[owners]) % TILES_DEV
        tiles = jnp.where(regular[chosen], regular_tile, random_tile).astype(jnp.int32)
        return (owners, tiles)
    owners, tiles = jax.vmap(one_device)(jnp.arange(DEVICES, dtype=jnp.int32))
    return (owners.reshape(NBLOCKS, 1).astype(jnp.int32), tiles.reshape(NBLOCKS).astype(jnp.int32))


def draw_owner_device(key, part):
    return remap_layout(jax.random.fold_in(key, 5))[0]


def draw_target_tile(key, part):
    return remap_layout(jax.random.fold_in(key, 5))[1]


def place_ends(array, key, low, high):
    place = [jax.random.randint(jax.random.fold_in(key, axis), (), 0, length) for axis, length in enumerate(array.shape)]
    longest = array.shape.index(max(array.shape))
    beside = place[:longest] + [(place[longest] + 1) % array.shape[longest]] + place[longest + 1:]
    return array.at[tuple(place)].set(low).at[tuple(beside)].set(high)


def levels(rng, dims, pieces, low, largest):
    factor_of, own = 1.0, jax.random.fold_in(rng, 6)
    for position, parts in pieces:
        draws = jnp.exp(jax.random.uniform(jax.random.fold_in(own, position), (parts,), jnp.float32, low / len(pieces), largest / len(pieces)))
        factor_of = factor_of * jnp.repeat(draws, dims[position] // parts).reshape([-1 if axis == position else 1 for axis in range(len(dims))])
    return factor_of


def centred(own_key, dims, width, most, split=(), kind=jnp.bfloat16):
    gain = levels(own_key, dims, split, -0.22, 0.18) if split else 1.0
    result = jax.random.normal(own_key, dims, jnp.float32) * width * gain
    return jnp.minimum(jnp.maximum(result, -most), most).astype(kind)


def setup_inputs(seed: int = 0) -> dict:
    splits = jax.random.split(jax.random.key(seed), 7)
    source = centred(splits[0], (LEV, NSRC), 1.0, 6.0, ((1, 256),))
    weights = centred(splits[1], (NBLOCKS, BLK, BLK), BLK ** -0.5, 0.5, ((0, 256),))
    source_block = place_ends(jax.random.randint(splits[2], (NBLOCKS,), 0, SB), jax.random.fold_in(splits[2], 1), 0, SB - 1).astype(jnp.int32)
    owner_device = draw_owner_device(jax.random.fold_in(splits[6], 71), 0)
    target_tile = draw_target_tile(jax.random.fold_in(splits[6], 71), 0)
    cutoff = place_ends(jax.random.randint(splits[5], (NLAT,), 1, KW), jax.random.fold_in(splits[5], 1), 1, KW - 1).astype(jnp.int32)
    return {"source": source, "weights": weights, "source_block": source_block, "owner_device": owner_device, "target_tile": target_tile, "cutoff": cutoff}


TWO_PI = 6.283185307179586


def zonal_table(start_index, length, period, wave_count):
    positions = start_index + lax.broadcasted_iota(jnp.int32, (length, wave_count), 0)
    wave_index = lax.broadcasted_iota(jnp.int32, (length, wave_count), 1)
    phases = (positions * wave_index) % period
    angles = phases.astype(jnp.float32) * (TWO_PI / period)
    return jnp.concatenate([jnp.cos(angles), jnp.sin(angles)], axis=1)


def spectral_weights(cutoffs, wave_count, period):
    wave_index = lax.broadcasted_iota(jnp.int32, (cutoffs.shape[0], wave_count), 1)
    scaled = jnp.where(wave_index == 0, 1.0, 2.0) / period
    retained = jnp.where(wave_index <= cutoffs[:, None], scaled, 0.0).astype(jnp.float32)
    return jnp.concatenate([retained, retained], axis=1)


def reference(source, weights, source_block, owner_device, target_tile, cutoff):
    device_total = N_BAND * N_COL
    blocks_all = source.reshape(LEV, device_total * SB, BLK)
    owners_all = owner_device[:, 0]

    def add_device(totals, device_index):
        first_block = device_index * NB
        block_weights = lax.dynamic_slice_in_dim(weights, first_block, NB, 0)
        chosen = lax.dynamic_slice_in_dim(source_block, first_block, NB, 0)
        owners = lax.dynamic_slice_in_dim(owners_all, first_block, NB, 0)
        tiles_hit = lax.dynamic_slice_in_dim(target_tile, first_block, NB, 0)
        picked = jnp.take(blocks_all, (device_index * SB + chosen).astype(jnp.int32), axis=1)
        partial_value = jnp.einsum("lnb,nbt->nlt", picked.astype(jnp.float32), block_weights.astype(jnp.float32))
        totals = totals.at[(owners * TILES_DEV + tiles_hit).astype(jnp.int32)].add(partial_value)
        return totals, None

    totals, unused = lax.scan(add_device, jnp.zeros((device_total * TILES_DEV, LEV, BLK), jnp.float32), jnp.arange(device_total, dtype=jnp.int32))
    cell_count = LATB * LON_DEV
    tiles = totals.reshape(N_BAND, N_COL, TILES_DEV, LEV, BLK)
    tiles = jnp.transpose(tiles, (3, 0, 1, 2, 4)).reshape(LEV, N_BAND, N_COL, TILES_DEV * BLK)[:, :, :, :cell_count]
    tiles = tiles.reshape(LEV, N_BAND, N_COL, LATB, LON_DEV)
    remapped = jnp.transpose(tiles, (0, 1, 3, 2, 4)).reshape(LEV, NLAT, NLON)
    wave_table = zonal_table(0, NLON, NLON, KW)
    spectrum = jnp.dot(remapped.reshape(LEV * NLAT, NLON), wave_table, precision=lax.Precision.HIGHEST, preferred_element_type=jnp.float32)
    spectrum = spectrum.reshape(LEV, NLAT, 2 * KW) * spectral_weights(cutoff, KW, NLON)[None]
    filtered = jnp.dot(spectrum.reshape(LEV * NLAT, 2 * KW), wave_table.T, precision=lax.Precision.HIGHEST, preferred_element_type=jnp.float32)
    return remapped, filtered.reshape(LEV, NLAT, NLON)
```

```python
import jax
import jax.numpy as jnp
from jax import lax
from jax.experimental import pallas as pl
from jax.experimental.pallas import tpu as pltpu
from jax.sharding import PartitionSpec as P

NLON = 7200
KW = 512
TWO_PI = 6.283185307179586

LEV = 6
BLK = 128
COLS = 32
LON = NLON // COLS
LATB = 64
CAP = 6
REG = 4
REG_ROWS = REG * LEV
OWN_ROWS = 16
NEAR_ROWS = 40
IRR_ROWS = 88
ID_ROW = 84
TILES = 128
P2_ROWS = 24
OWN_ID = (CAP - REG) * LEV
UP_LANE = REG * LEV
DOWN_LANE = UP_LANE + CAP * LEV
OWN_LANE = DOWN_LANE + CAP * LEV
CHUNK = 64
CHUNKS = 4
AXES = True


def split2(x):
    hi = x.astype(jnp.bfloat16)
    lo = (x - hi.astype(jnp.float32)).astype(jnp.bfloat16)
    return hi, lo


def dot32(a, b):
    return jnp.dot(a, b, preferred_element_type=jnp.float32)


def dot3(a, b):
    return dot32(a[0], b[0]) + (dot32(a[0], b[1]) + dot32(a[1], b[0]))


def place_kernel(sb_hbm, owner_hbm, tile_hbm, src_hbm, w_hbm, reg_hbm, own_hbm, up_hbm, down_hbm, w, src, sb, owners, tiles, buf, marks, count, w_sem, in_sem, out_sem):
    def chunk_copy(i):
        part = pl.ds(i * CHUNK, CHUNK)
        return pltpu.make_async_copy(w_hbm.at[part], w.at[part], w_sem.at[i])

    small = [
        pltpu.make_async_copy(owner_hbm, owners, in_sem.at[0]),
        pltpu.make_async_copy(sb_hbm, sb, in_sem.at[1]),
        pltpu.make_async_copy(tile_hbm, tiles, in_sem.at[2]),
        pltpu.make_async_copy(src_hbm, src, in_sem.at[3]),
    ]
    for copy in small:
        copy.start()
    for i in range(CHUNKS):
        chunk_copy(i).start()
    for i in range(3 * COLS):
        count[i] = 0
    buf[...] = jnp.zeros_like(buf)
    marks[...] = jnp.zeros_like(marks)
    for copy in small:
        copy.wait()
    lane = lax.broadcasted_iota(jnp.int32, (1, BLK), 1)
    first = ((lax.axis_index("band").astype(jnp.int32) if AXES else 3) - 1) * COLS

    def chunk(i, carry):
        chunk_copy(i).wait()
        for u in range(CHUNK):
            n = i * CHUNK + u
            key = owners[n] - first
            start = pl.multiple_of(sb[n] * BLK, BLK)
            value = dot32(src[:, pl.ds(start, BLK)], w[n])
            row = count[key]
            count[key] = row + LEV
            buf[key, pl.ds(row, LEV), :] = value
            at = lane - row
            mark = jnp.where((at >= 0) & (at < LEV), at * TILES + (tiles[n] + 1), 0)
            marks[pl.ds(key, 1), :] = marks[pl.ds(key, 1), :] + mark.astype(jnp.float32)
        return carry

    lax.fori_loop(0, CHUNKS, chunk, 0)
    near = pl.ds(0, COLS)
    own = pl.ds(COLS, COLS)
    below, mine, above = marks[:COLS, :], marks[COLS : 2 * COLS, :], marks[2 * COLS :, :]
    mine = jnp.where(lane < REG_ROWS, mine, 0.0) + jnp.where(
        lane >= OWN_LANE, pltpu.roll(mine, OWN_LANE - REG_ROWS, 1), 0.0
    )
    marks[:COLS, :] = pltpu.roll(below, DOWN_LANE, 1)
    marks[COLS : 2 * COLS, :] = mine
    marks[2 * COLS :, :] = pltpu.roll(above, UP_LANE, 1)
    for key in range(3 * COLS):
        buf[key, CAP * LEV : CAP * LEV + 1, :] = marks[key : key + 1, :]
    parts = (
        (buf.at[pl.ds(2 * COLS, COLS)], up_hbm),
        (buf.at[near], down_hbm),
        (buf.at[own, pl.ds(0, REG_ROWS)], reg_hbm),
        (buf.at[own, pl.ds(REG_ROWS, OWN_ROWS)], own_hbm),
    )
    copies = [pltpu.make_async_copy(part, ref, out_sem.at[i]) for i, (part, ref) in enumerate(parts)]
    for copy in copies:
        copy.start()
    for copy in copies:
        copy.wait()


def place(source, weights, source_block, owners, target_tile, interpret=False):
    hbm = pl.BlockSpec(memory_space=pltpu.HBM)
    blocks = weights.shape[0]
    kinds = (REG_ROWS, OWN_ROWS, NEAR_ROWS, NEAR_ROWS)
    return pl.pallas_call(
        place_kernel,
        out_shape=[jax.ShapeDtypeStruct((COLS, r, BLK), jnp.float32) for r in kinds],
        in_specs=[hbm] * 5,
        out_specs=[hbm] * 4,
        scratch_shapes=[
            pltpu.VMEM(weights.shape, weights.dtype),
            pltpu.VMEM(source.shape, source.dtype),
            pltpu.SMEM((blocks,), jnp.int32),
            pltpu.SMEM((blocks,), jnp.int32),
            pltpu.SMEM((blocks,), jnp.int32),
            pltpu.VMEM((3 * COLS, NEAR_ROWS, BLK), jnp.float32),
            pltpu.VMEM((3 * COLS, BLK), jnp.float32),
            pltpu.SMEM((3 * COLS,), jnp.int32),
            pltpu.SemaphoreType.DMA((CHUNKS,)),
            pltpu.SemaphoreType.DMA((4,)),
            pltpu.SemaphoreType.DMA((4,)),
        ],
        compiler_params=pltpu.CompilerParams(vmem_limit_bytes=58 << 20),
        cost_estimate=pl.CostEstimate(flops=100_000_000, bytes_accessed=10_000_000, transcendentals=0),
        interpret=interpret,
        name="place",
    )(source_block, owners, target_tile, source, weights)


def join_kernel(own_ref, below_ref, above_ref, irr_ref):
    near = CAP * LEV
    for c in range(COLS):
        irr_ref[c, :near, :] = below_ref[c, :near, :]
        irr_ref[c, near : 2 * near, :] = above_ref[c, :near, :]
        irr_ref[c, 2 * near :, :] = own_ref[c]
        ids = own_ref[c, OWN_ID : OWN_ID + 1, :] + below_ref[c, near : near + 1, :] + above_ref[c, near : near + 1, :]
        irr_ref[c, ID_ROW : ID_ROW + 1, :] = ids


def join(own, below, above, interpret=False):
    return pl.pallas_call(
        join_kernel,
        out_shape=jax.ShapeDtypeStruct((COLS, IRR_ROWS, BLK), jnp.float32),
        cost_estimate=pl.CostEstimate(flops=1_000_000, bytes_accessed=3_000_000, transcendentals=0),
        compiler_params=pltpu.CompilerParams(vmem_limit_bytes=12 << 20),
        interpret=interpret,
        name="join",
    )(own, below, above)


def combine_kernel(reg_ref, irr_ref, out_ref, acc, sums):
    rows = lax.broadcasted_iota(jnp.int32, (LEV * TILES, 2 * BLK), 0).astype(jnp.float32) + 1.0
    pad = jnp.zeros((BLK - REG_ROWS - IRR_ROWS, BLK), jnp.float32)
    for s in range(0, COLS, 2):
        data = jnp.concatenate([reg_ref[s], irr_ref[s], pad, reg_ref[s + 1], irr_ref[s + 1], pad], axis=0)
        ids = jnp.concatenate([irr_ref[s, ID_ROW : ID_ROW + 1, :], irr_ref[s + 1, ID_ROW : ID_ROW + 1, :]], axis=1)
        chooser = jnp.where(rows == ids, 1.0, 0.0).astype(jnp.bfloat16)
        both = jnp.concatenate(split2(data), axis=1)
        part = dot32(chooser, both)
        if s == 0:
            acc[...] = part
        else:
            acc[...] += part
    sums[...] = acc[:, :BLK] + acc[:, BLK:]
    lane = lax.broadcasted_iota(jnp.int32, (LEV, BLK), 1)
    for lat in range(LATB):
        for half in range(2):
            first, shift = divmod(lat * LON + half * BLK, BLK)
            value = sums[pl.ds(first, LEV, stride=TILES), :]
            if shift:
                later = sums[pl.ds(first + 1, LEV, stride=TILES), :]
                value = jnp.where(lane < BLK - shift, pltpu.roll(value, BLK - shift, 1), pltpu.roll(later, BLK - shift, 1))
            at = (lat % 2) * 2 * LEV + half * LEV
            out_ref[lat // 2, at : at + LEV, :] = value


def combine(reg, irr, interpret=False):
    return pl.pallas_call(
        combine_kernel,
        out_shape=jax.ShapeDtypeStruct((COLS, P2_ROWS, BLK), jnp.float32),
        scratch_shapes=[
            pltpu.VMEM((LEV * TILES, 2 * BLK), jnp.float32),
            pltpu.VMEM((LEV * TILES, BLK), jnp.float32),
        ],
        compiler_params=pltpu.CompilerParams(vmem_limit_bytes=24 << 20),
        cost_estimate=pl.CostEstimate(flops=1_600_000_000, bytes_accessed=2_000_000, transcendentals=0),
        interpret=interpret,
        name="combine",
    )(reg, irr)


def filter_kernel(cut_ref, x_ref, f_ref, ft_ref, g_ref, gt_ref, tc_ref, ts_ref, out_ref):
    lat_count = 2
    pieces = []
    for p in range(lat_count):
        for l in range(LEV):
            for h in range(2):
                pieces.append(x_ref[pl.ds(p * 2 * LEV + h * LEV + l, COLS, stride=P2_ROWS), :])
    x = jnp.concatenate(pieces, axis=1)
    f = (f_ref[0], f_ref[1])
    ft = (ft_ref[0], ft_ref[1])
    g = (g_ref[0], g_ref[1])
    gt = (gt_ref[0], gt_ref[1])
    tc, ts = tc_ref[...], ts_ref[...]
    y = dot3(f, split2(x))
    rows = []
    for r in range(lat_count * LEV):
        re, im = y[:COLS, r * 256 : r * 256 + 256], y[COLS:, r * 256 : r * 256 + 256]
        rows.append(jnp.concatenate([re * tc + im * ts, im * tc - re * ts], axis=1))
    u = jnp.concatenate(rows, axis=0)
    z = dot3(split2(u), g)
    row = lax.broadcasted_iota(jnp.int32, z.shape, 0)
    m = lax.broadcasted_iota(jnp.int32, z.shape, 1) % (KW // COLS)
    k = row % COLS + COLS * m
    cut = jnp.where(row < LEV * COLS, cut_ref[0], cut_ref[1])
    gain = jnp.where(k == 0, 1.0 / NLON, 2.0 / NLON)
    z = z * jnp.where(k <= cut, gain, 0.0)
    w = dot3(split2(z), gt)
    cols = []
    for r in range(lat_count * LEV):
        part = w[r * COLS : r * COLS + COLS]
        re, im = part[:, :256], part[:, 256:]
        cols.append(jnp.concatenate([re * tc - im * ts, re * ts + im * tc], axis=0))
    v = jnp.concatenate(cols, axis=1)
    out = dot3(ft, split2(v))
    at = 0
    for p in range(lat_count):
        for l in range(LEV):
            for h in range(2):
                out_ref[pl.ds(p * 2 * LEV + h * LEV + l, COLS, stride=P2_ROWS), :] = out[:, at * BLK : at * BLK + BLK]
                at += 1


def zonal_filter(rows, cutoff, tables, interpret=False):
    vmem = pl.BlockSpec(memory_space=pltpu.VMEM)
    out = pl.pallas_call(
        filter_kernel,
        out_shape=jax.ShapeDtypeStruct((COLS * P2_ROWS, BLK), jnp.float32),
        in_specs=[pl.BlockSpec(memory_space=pltpu.SMEM)] + [vmem] * 7,
        out_specs=vmem,
        compiler_params=pltpu.CompilerParams(vmem_limit_bytes=24 << 20),
        cost_estimate=pl.CostEstimate(flops=300_000_000, bytes_accessed=1_000_000, transcendentals=0),
        interpret=interpret,
        name="zonal",
    )(cutoff, rows.reshape(COLS * P2_ROWS, BLK), *tables)
    return out.reshape(COLS, P2_ROWS, BLK)


def angles(shape, factor, period):
    a = lax.broadcasted_iota(jnp.int32, shape, 0)
    b = lax.broadcasted_iota(jnp.int32, shape, 1)
    phases = a * b * factor % period
    return phases.astype(jnp.float32) * (TWO_PI / period)


def stack2(x):
    hi = lax.reduce_precision(x, 8, 7)
    return jnp.stack([hi.astype(jnp.bfloat16), (x - hi).astype(jnp.bfloat16)])


def zonal_tables():
    theta = angles((COLS, COLS), 1, COLS)
    f = jnp.concatenate([jnp.cos(theta), -jnp.sin(theta)], axis=0)
    turn = angles((COLS, 256), 1, NLON)
    tc, ts = jnp.cos(turn), jnp.sin(turn)
    phi = angles((KW // COLS, 256), COLS, NLON)
    inside = lax.broadcasted_iota(jnp.int32, phi.shape, 1) < LON
    c, s = jnp.where(inside, jnp.cos(phi), 0.0), jnp.where(inside, jnp.sin(phi), 0.0)
    gt = jnp.concatenate([jnp.concatenate([c, s], axis=1), jnp.concatenate([-s, c], axis=1)], axis=0)
    return stack2(f), stack2(f.T), stack2(gt.T), stack2(gt), tc, ts


def lay_kernel(rows_ref, out_ref, low, high):
    for h, half in enumerate((low, high)):
        for p in range(2):
            for l in range(LEV):
                part = rows_ref[pl.ds(p * 2 * LEV + h * LEV + l, COLS, stride=P2_ROWS), :]
                half[pl.ds(l * LATB + p, COLS, stride=2), :] = part
    for l in range(LEV):
        out_ref[l, :, :BLK] = low[l * LATB : l * LATB + LATB, :]
        out_ref[l, :, BLK:] = high[l * LATB : l * LATB + LATB, : LON - BLK]


def by_latitude(rows, interpret=False):
    return pl.pallas_call(
        lay_kernel,
        out_shape=jax.ShapeDtypeStruct((LEV, LATB, LON), jnp.float32),
        scratch_shapes=[pltpu.VMEM((LEV * LATB, BLK), jnp.float32)] * 2,
        cost_estimate=pl.CostEstimate(flops=1_000_000, bytes_accessed=800_000, transcendentals=0),
        compiler_params=pltpu.CompilerParams(vmem_limit_bytes=8 << 20),
        interpret=interpret,
        name="lay",
    )(rows.reshape(COLS * P2_ROWS, BLK))


def exchange(array):
    return lax.all_to_all(array, "col", 0, 0, tiled=True)


def local(source, weights, source_block, owner_device, target_tile, cutoff):
    bands = lax.axis_size("band")
    reg, own, up, down = place(source, weights, source_block, owner_device[:, 0], target_tile)
    steps = [(i, i + 1) for i in range(bands - 1)]
    below = lax.ppermute(up, "band", steps)
    above = lax.ppermute(down, "band", [(j, i) for i, j in steps])
    reg = exchange(reg)
    irr = exchange(join(own, below, above))
    rows = combine(reg, irr)
    remapped = by_latitude(rows)
    rows = exchange(rows)
    rows = zonal_filter(rows, cutoff, zonal_tables())
    filtered = by_latitude(exchange(rows))
    return (remapped, filtered)


def solution(mesh):
    in_specs = (
        P(None, ("band", "col")),
        P(("band", "col"), None, None),
        P(("band", "col")),
        P(("band", "col"), None),
        P(("band", "col")),
        P(("band", "col")),
    )
    out_specs = (P(None, "band", "col"), P(None, "band", "col"))
    return jax.shard_map(local, mesh=mesh, in_specs=in_specs, out_specs=out_specs, check_vma=False)
```

```python
import jax
import jax.numpy as jnp
from jax import lax
from jax.experimental import pallas as pl
from jax.experimental.pallas import tpu as pltpu
from jax.sharding import PartitionSpec as P

NLON = 7200
KW = 512
TWO_PI = 6.283185307179586

LEV = 6
BLK = 128
COLS = 32
LON = NLON // COLS
LATB = 64
CAP = 6
SIDE_ROWS = CAP * LEV
ID_ROW = 3 * SIDE_ROWS
ROWS = ID_ROW + 4
WINDOW = 8
TILES = 120
P2_ROWS = 24
CHUNK = 64
CHUNKS = 4
AXES = True


def split2(x):
    hi = x.astype(jnp.bfloat16)
    lo = (x - hi.astype(jnp.float32)).astype(jnp.bfloat16)
    return hi, lo


def dot32(a, b):
    return jnp.dot(a, b, preferred_element_type=jnp.float32)


def dot3(a, b):
    return dot32(a[0], b[0]) + (dot32(a[0], b[1]) + dot32(a[1], b[0]))


def place_kernel(sb_hbm, owner_hbm, tile_hbm, src_hbm, w_hbm, out_hbm, w, src, sb, owners, tiles, buf, marks, count, w_sem, in_sem, out_sem):
    def chunk_copy(i):
        part = pl.ds(i * CHUNK, CHUNK)
        return pltpu.make_async_copy(w_hbm.at[part], w.at[part], w_sem.at[i])

    small = [
        pltpu.make_async_copy(owner_hbm, owners, in_sem.at[0]),
        pltpu.make_async_copy(sb_hbm, sb, in_sem.at[1]),
        pltpu.make_async_copy(tile_hbm, tiles, in_sem.at[2]),
        pltpu.make_async_copy(src_hbm, src, in_sem.at[3]),
    ]
    for copy in small:
        copy.start()
    for i in range(CHUNKS):
        chunk_copy(i).start()
    for i in range(3 * COLS):
        count[i] = 0
    buf[...] = jnp.zeros_like(buf)
    marks[...] = jnp.zeros_like(marks)
    for copy in small:
        copy.wait()
    band = lax.axis_index("band").astype(jnp.int32) if AXES else 3
    col = lax.axis_index("col").astype(jnp.int32) if AXES else 5
    first = (band - 1) * COLS
    odd = band % 2
    side_base = jnp.where(odd == 1, 0, 2 * SIDE_ROWS)
    side_step = jnp.where(odd == 1, SIDE_ROWS, -SIDE_ROWS)
    lane = (lax.broadcasted_iota(jnp.int32, (1, BLK), 1) - col % (COLS // 2) * WINDOW) * LEV

    def chunk(i, carry):
        chunk_copy(i).wait()
        for u in range(CHUNK):
            n = i * CHUNK + u
            key = owners[n] - first
            start = pl.multiple_of(sb[n] * BLK, BLK)
            value = dot32(src[:, pl.ds(start, BLK)], w[n])
            row = count[key]
            count[key] = row + LEV
            buf[key & (COLS - 1), pl.ds((key >> 5) * side_step + (side_base + row), LEV), :] = value
            mark = jnp.where(lane == row, tiles[n] + 1, 0)
            marks[pl.ds(key, 1), :] = marks[pl.ds(key, 1), :] + mark.astype(jnp.float32)
        return carry

    lax.fori_loop(0, CHUNKS, chunk, 0)
    below, above = marks[:COLS, :], marks[2 * COLS :, :]
    marks[:COLS, :] = jnp.where(odd == 1, below, above)
    marks[2 * COLS :, :] = pltpu.roll(jnp.where(odd == 1, above, below), WINDOW - CAP, 1)
    for key in range(3 * COLS):
        row = ID_ROW + key // COLS
        buf[key % COLS, row : row + 1, :] = marks[key : key + 1, :]
    out = pltpu.make_async_copy(buf, out_hbm, out_sem)
    out.start()
    out.wait()


def place(source, weights, source_block, owners, target_tile, interpret=False):
    hbm = pl.BlockSpec(memory_space=pltpu.HBM)
    blocks = weights.shape[0]
    return pl.pallas_call(
        place_kernel,
        out_shape=jax.ShapeDtypeStruct((COLS, ROWS, BLK), jnp.float32),
        in_specs=[hbm] * 5,
        out_specs=hbm,
        scratch_shapes=[
            pltpu.VMEM(weights.shape, weights.dtype),
            pltpu.VMEM(source.shape, source.dtype),
            pltpu.SMEM((blocks,), jnp.int32),
            pltpu.SMEM((blocks,), jnp.int32),
            pltpu.SMEM((blocks,), jnp.int32),
            pltpu.VMEM((COLS, ROWS, BLK), jnp.float32),
            pltpu.VMEM((3 * COLS, BLK), jnp.float32),
            pltpu.SMEM((3 * COLS,), jnp.int32),
            pltpu.SemaphoreType.DMA((CHUNKS,)),
            pltpu.SemaphoreType.DMA((4,)),
            pltpu.SemaphoreType.DMA,
        ],
        compiler_params=pltpu.CompilerParams(vmem_limit_bytes=58 << 20),
        cost_estimate=pl.CostEstimate(flops=100_000_000, bytes_accessed=10_000_000, transcendentals=0),
        interpret=interpret,
        name="place",
    )(source_block, owners, target_tile, source, weights)


def sum_side(side, got_ref, out_ref):
    begin = min(side * CAP, 3 * CAP - WINDOW) * LEV
    halves = []
    for half in range(2):
        at = half * (COLS // 2) * ROWS + ID_ROW + side
        marks = [got_ref[pl.ds(at + g * 8 * ROWS, 8, stride=ROWS), :] for g in range(2)]
        halves.append(jnp.sum(marks[0] + marks[1], axis=0, keepdims=True))
    ids = jnp.concatenate(halves, axis=1)
    tile = lax.broadcasted_iota(jnp.int32, (TILES, 2 * BLK), 0).astype(jnp.float32) + 1.0
    chooser = jnp.where(tile == ids, 1.0, 0.0).astype(jnp.bfloat16)
    for l in range(LEV):
        data = [got_ref[pl.ds(s * ROWS + begin + l, WINDOW, stride=LEV), :] for s in range(COLS)]
        both = dot32(chooser, jnp.concatenate(split2(jnp.concatenate(data, axis=0)), axis=1))
        out_ref[l * TILES : l * TILES + TILES, :] = both[:, :BLK] + both[:, BLK:]


def tile_sums(got, side, interpret=False):
    return pl.pallas_call(
        lambda got_ref, out_ref: sum_side(side, got_ref, out_ref),
        out_shape=jax.ShapeDtypeStruct((LEV * TILES, BLK), jnp.float32),
        compiler_params=pltpu.CompilerParams(vmem_limit_bytes=24 << 20),
        cost_estimate=pl.CostEstimate(flops=100_000_000, bytes_accessed=1_000_000, transcendentals=0),
        interpret=interpret,
        name=("core", "own", "chip")[side],
    )(got)


def by_row_kernel(own_ref, core_ref, chip_ref, out_ref, sums):
    sums[...] = own_ref[...] + core_ref[...] + chip_ref[...]
    lane = lax.broadcasted_iota(jnp.int32, (LEV, BLK), 1)
    for lat in range(LATB):
        for half in range(2):
            first, shift = divmod(lat * LON + half * BLK, BLK)
            value = sums[pl.ds(first, LEV, stride=TILES), :]
            if shift:
                later = sums[pl.ds(first + 1, LEV, stride=TILES), :]
                value = jnp.where(lane < BLK - shift, pltpu.roll(value, BLK - shift, 1), pltpu.roll(later, BLK - shift, 1))
            at = (lat % 2) * 2 * LEV + half * LEV
            out_ref[lat // 2, at : at + LEV, :] = value


def by_row(own, core, chip, interpret=False):
    return pl.pallas_call(
        by_row_kernel,
        out_shape=jax.ShapeDtypeStruct((COLS, P2_ROWS, BLK), jnp.float32),
        scratch_shapes=[pltpu.VMEM((LEV * TILES, BLK), jnp.float32)],
        compiler_params=pltpu.CompilerParams(vmem_limit_bytes=12 << 20),
        cost_estimate=pl.CostEstimate(flops=1_000_000, bytes_accessed=1_500_000, transcendentals=0),
        interpret=interpret,
        name="by_row",
    )(own, core, chip)


def filter_kernel(cut_ref, x_ref, f_ref, ft_ref, g_ref, gt_ref, tc_ref, ts_ref, out_ref):
    lat_count = 2
    pieces = []
    for p in range(lat_count):
        for l in range(LEV):
            for h in range(2):
                pieces.append(x_ref[pl.ds(p * 2 * LEV + h * LEV + l, COLS, stride=P2_ROWS), :])
    x = jnp.concatenate(pieces, axis=1)
    f = (f_ref[0], f_ref[1])
    ft = (ft_ref[0], ft_ref[1])
    g = (g_ref[0], g_ref[1])
    gt = (gt_ref[0], gt_ref[1])
    tc, ts = tc_ref[...], ts_ref[...]
    y = dot3(f, split2(x))
    rows = []
    for r in range(lat_count * LEV):
        re, im = y[:COLS, r * 256 : r * 256 + 256], y[COLS:, r * 256 : r * 256 + 256]
        rows.append(jnp.concatenate([re * tc + im * ts, im * tc - re * ts], axis=1))
    u = jnp.concatenate(rows, axis=0)
    z = dot3(split2(u), g)
    row = lax.broadcasted_iota(jnp.int32, z.shape, 0)
    m = lax.broadcasted_iota(jnp.int32, z.shape, 1) % (KW // COLS)
    k = row % COLS + COLS * m
    cut = jnp.where(row < LEV * COLS, cut_ref[0], cut_ref[1])
    gain = jnp.where(k == 0, 1.0 / NLON, 2.0 / NLON)
    z = z * jnp.where(k <= cut, gain, 0.0)
    w = dot3(split2(z), gt)
    cols = []
    for r in range(lat_count * LEV):
        part = w[r * COLS : r * COLS + COLS]
        re, im = part[:, :256], part[:, 256:]
        cols.append(jnp.concatenate([re * tc - im * ts, re * ts + im * tc], axis=0))
    v = jnp.concatenate(cols, axis=1)
    out = dot3(ft, split2(v))
    at = 0
    for p in range(lat_count):
        for l in range(LEV):
            for h in range(2):
                out_ref[pl.ds(p * 2 * LEV + h * LEV + l, COLS, stride=P2_ROWS), :] = out[:, at * BLK : at * BLK + BLK]
                at += 1


def zonal_filter(rows, cutoff, tables, interpret=False):
    vmem = pl.BlockSpec(memory_space=pltpu.VMEM)
    out = pl.pallas_call(
        filter_kernel,
        out_shape=jax.ShapeDtypeStruct((COLS * P2_ROWS, BLK), jnp.float32),
        in_specs=[pl.BlockSpec(memory_space=pltpu.SMEM)] + [vmem] * 7,
        out_specs=vmem,
        compiler_params=pltpu.CompilerParams(vmem_limit_bytes=24 << 20),
        cost_estimate=pl.CostEstimate(flops=300_000_000, bytes_accessed=1_000_000, transcendentals=0),
        interpret=interpret,
        name="zonal",
    )(cutoff, rows.reshape(COLS * P2_ROWS, BLK), *tables)
    return out.reshape(COLS, P2_ROWS, BLK)


def angles(shape, factor, period):
    a = lax.broadcasted_iota(jnp.int32, shape, 0)
    b = lax.broadcasted_iota(jnp.int32, shape, 1)
    phases = a * b * factor % period
    return phases.astype(jnp.float32) * (TWO_PI / period)


def stack2(x):
    hi = lax.reduce_precision(x, 8, 7)
    return jnp.stack([hi.astype(jnp.bfloat16), (x - hi).astype(jnp.bfloat16)])


def zonal_tables():
    theta = angles((COLS, COLS), 1, COLS)
    f = jnp.concatenate([jnp.cos(theta), -jnp.sin(theta)], axis=0)
    turn = angles((COLS, 256), 1, NLON)
    tc, ts = jnp.cos(turn), jnp.sin(turn)
    phi = angles((KW // COLS, 256), COLS, NLON)
    inside = lax.broadcasted_iota(jnp.int32, phi.shape, 1) < LON
    c, s = jnp.where(inside, jnp.cos(phi), 0.0), jnp.where(inside, jnp.sin(phi), 0.0)
    gt = jnp.concatenate([jnp.concatenate([c, s], axis=1), jnp.concatenate([-s, c], axis=1)], axis=0)
    return stack2(f), stack2(f.T), stack2(gt.T), stack2(gt), tc, ts


def lay_kernel(rows_ref, out_ref, low, high):
    for h, half in enumerate((low, high)):
        for p in range(2):
            for l in range(LEV):
                part = rows_ref[pl.ds(p * 2 * LEV + h * LEV + l, COLS, stride=P2_ROWS), :]
                half[pl.ds(l * LATB + p, COLS, stride=2), :] = part
    for l in range(LEV):
        out_ref[l, :, :BLK] = low[l * LATB : l * LATB + LATB, :]
        out_ref[l, :, BLK:] = high[l * LATB : l * LATB + LATB, : LON - BLK]


def by_latitude(rows, interpret=False):
    return pl.pallas_call(
        lay_kernel,
        out_shape=jax.ShapeDtypeStruct((LEV, LATB, LON), jnp.float32),
        scratch_shapes=[pltpu.VMEM((LEV * LATB, BLK), jnp.float32)] * 2,
        cost_estimate=pl.CostEstimate(flops=1_000_000, bytes_accessed=800_000, transcendentals=0),
        compiler_params=pltpu.CompilerParams(vmem_limit_bytes=8 << 20),
        interpret=interpret,
        name="lay",
    )(rows.reshape(COLS * P2_ROWS, BLK))


def exchange(array):
    return lax.all_to_all(array, "col", 0, 0, tiled=True)


def local(source, weights, source_block, owner_device, target_tile, cutoff):
    bands = lax.axis_size("band")
    got = exchange(place(source, weights, source_block, owner_device[:, 0], target_tile))
    got = got.reshape(COLS * ROWS, BLK)
    chip = lax.ppermute(tile_sums(got, 2), "band", [(i, i + 1 if i % 2 else i - 1) for i in range(1, bands - 1)])
    core = lax.ppermute(tile_sums(got, 0), "band", [(i, i ^ 1) for i in range(bands)])
    rows = by_row(tile_sums(got, 1), core, chip)
    remapped = by_latitude(rows)
    rows = exchange(rows)
    rows = zonal_filter(rows, cutoff, zonal_tables())
    filtered = by_latitude(exchange(rows))
    return (remapped, filtered)


def solution(mesh):
    in_specs = (
        P(None, ("band", "col")),
        P(("band", "col"), None, None),
        P(("band", "col")),
        P(("band", "col"), None),
        P(("band", "col")),
        P(("band", "col")),
    )
    out_specs = (P(None, "band", "col"), P(None, "band", "col"))
    return jax.shard_map(local, mesh=mesh, in_specs=in_specs, out_specs=out_specs, check_vma=False)
```

```python
import jax
import jax.numpy as jnp
from jax import lax
from jax.experimental import pallas as pl
from jax.experimental.pallas import tpu as pltpu
from jax.sharding import PartitionSpec as P

NLON = 7200
KW = 512
TWO_PI = 6.283185307179586

LEV = 6
BLK = 128
COLS = 32
LON = NLON // COLS
LATB = 64
CAP = 6
SIDE_ROWS = CAP * LEV
ID_ROW = 3 * SIDE_ROWS
ROWS = ID_ROW + 4
WINDOW = 8
TILES = 120
P2_ROWS = 24
CHUNK = 128
CHUNKS = 2
AXES = True


def split2(x):
    hi = x.astype(jnp.bfloat16)
    lo = (x - hi.astype(jnp.float32)).astype(jnp.bfloat16)
    return hi, lo


def dot32(a, b):
    return jnp.dot(a, b, preferred_element_type=jnp.float32)


def place_kernel(sb_hbm, owner_hbm, tile_hbm, src_hbm, w_hbm, buf, w, src, sb, owners, tiles, marks, count, w_sem, in_sem):
    def chunk_copy(i):
        part = pl.ds(i * CHUNK, CHUNK)
        return pltpu.make_async_copy(w_hbm.at[part], w.at[part], w_sem.at[i])

    small = [
        pltpu.make_async_copy(owner_hbm, owners, in_sem.at[0]),
        pltpu.make_async_copy(sb_hbm, sb, in_sem.at[1]),
        pltpu.make_async_copy(tile_hbm, tiles, in_sem.at[2]),
        pltpu.make_async_copy(src_hbm, src, in_sem.at[3]),
    ]
    for copy in small:
        copy.start()
    for i in range(CHUNKS):
        chunk_copy(i).start()
    for i in range(3 * COLS):
        count[i] = 0
    buf[...] = jnp.zeros_like(buf)
    marks[...] = jnp.zeros_like(marks)
    for copy in small:
        copy.wait()
    band = lax.axis_index("band").astype(jnp.int32) if AXES else 3
    col = lax.axis_index("col").astype(jnp.int32) if AXES else 5
    first = (band - 1) * COLS
    odd = band % 2
    side_base = jnp.where(odd == 1, 0, 2 * SIDE_ROWS)
    side_step = jnp.where(odd == 1, SIDE_ROWS, -SIDE_ROWS)
    lane = (lax.broadcasted_iota(jnp.int32, (1, BLK), 1) - col % (COLS // 2) * WINDOW) * LEV

    def chunk(i, carry):
        chunk_copy(i).wait()
        for u in range(CHUNK):
            n = i * CHUNK + u
            key = owners[n] - first
            start = pl.multiple_of(sb[n] * BLK, BLK)
            value = dot32(src[:, pl.ds(start, BLK)], w[n])
            row = count[key]
            count[key] = row + LEV
            buf[key & (COLS - 1), pl.ds((key >> 5) * side_step + (side_base + row), LEV), :] = value
            mark = jnp.where(lane == row, tiles[n] + 1, 0)
            marks[pl.ds(key, 1), :] = marks[pl.ds(key, 1), :] + mark.astype(jnp.float32)
        return carry

    lax.fori_loop(0, CHUNKS, chunk, 0)
    below, above = marks[:COLS, :], marks[2 * COLS :, :]
    marks[:COLS, :] = jnp.where(odd == 1, below, above)
    marks[2 * COLS :, :] = pltpu.roll(jnp.where(odd == 1, above, below), WINDOW - CAP, 1)
    for key in range(3 * COLS):
        row = ID_ROW + key // COLS
        buf[key % COLS, row : row + 1, :] = marks[key : key + 1, :]


def place(source, weights, source_block, owners, target_tile, interpret=False):
    hbm = pl.BlockSpec(memory_space=pltpu.HBM)
    blocks = weights.shape[0]
    return pl.pallas_call(
        place_kernel,
        out_shape=pltpu.VMEM((COLS, ROWS, BLK), jnp.float32),
        in_specs=[hbm] * 5,
        out_specs=pl.BlockSpec(memory_space=pltpu.VMEM),
        scratch_shapes=[
            pltpu.VMEM(weights.shape, weights.dtype),
            pltpu.VMEM(source.shape, source.dtype),
            pltpu.SMEM((blocks,), jnp.int32),
            pltpu.SMEM((blocks,), jnp.int32),
            pltpu.SMEM((blocks,), jnp.int32),
            pltpu.VMEM((3 * COLS, BLK), jnp.float32),
            pltpu.SMEM((3 * COLS,), jnp.int32),
            pltpu.SemaphoreType.DMA((CHUNKS,)),
            pltpu.SemaphoreType.DMA((4,)),
        ],
        compiler_params=pltpu.CompilerParams(vmem_limit_bytes=58 << 20),
        cost_estimate=pl.CostEstimate(flops=100_000_000, bytes_accessed=10_000_000, transcendentals=0),
        interpret=interpret,
        name="place",
    )(source_block, owners, target_tile, source, weights)


def sum_side(side, got_ref, out_ref):
    begin = min(side * CAP, 3 * CAP - WINDOW) * LEV
    halves = []
    for half in range(2):
        at = half * (COLS // 2) * ROWS + ID_ROW + side
        marks = [got_ref[pl.ds(at + g * 8 * ROWS, 8, stride=ROWS), :] for g in range(2)]
        halves.append(jnp.sum(marks[0] + marks[1], axis=0, keepdims=True))
    ids = jnp.concatenate(halves, axis=1)
    tile = lax.broadcasted_iota(jnp.int32, (TILES, 2 * BLK), 0).astype(jnp.float32) + 1.0
    chooser = jnp.where(tile == ids, 1.0, 0.0).astype(jnp.bfloat16)
    for l in range(LEV):
        data = [got_ref[pl.ds(s * ROWS + begin + l, WINDOW, stride=LEV), :] for s in range(COLS)]
        both = dot32(chooser, jnp.concatenate(split2(jnp.concatenate(data, axis=0)), axis=1))
        out_ref[l * TILES : l * TILES + TILES, :] = both[:, :BLK] + both[:, BLK:]


def tile_sums(got, sides, interpret=False):
    def kernel(got_ref, *out_refs):
        for side, out_ref in zip(sides, out_refs):
            sum_side(side, got_ref, out_ref)

    return pl.pallas_call(
        kernel,
        out_shape=[jax.ShapeDtypeStruct((LEV * TILES, BLK), jnp.float32)] * len(sides),
        compiler_params=pltpu.CompilerParams(vmem_limit_bytes=24 << 20),
        cost_estimate=pl.CostEstimate(flops=100_000_000 * len(sides), bytes_accessed=1_000_000, transcendentals=0),
        interpret=interpret,
    )(got)


def by_row_kernel(own_ref, core_ref, chip_ref, out_ref, sums):
    sums[...] = own_ref[...] + core_ref[...] + chip_ref[...]
    lane = lax.broadcasted_iota(jnp.int32, (LEV, BLK), 1)
    for lat in range(LATB):
        for half in range(2):
            first, shift = divmod(lat * LON + half * BLK, BLK)
            value = sums[pl.ds(first, LEV, stride=TILES), :]
            if shift:
                later = sums[pl.ds(first + 1, LEV, stride=TILES), :]
                value = jnp.where(lane < BLK - shift, pltpu.roll(value, BLK - shift, 1), pltpu.roll(later, BLK - shift, 1))
            at = (lat % 2) * 2 * LEV + half * LEV
            out_ref[lat // 2, at : at + LEV, :] = value


def by_row(own, core, chip, interpret=False):
    return pl.pallas_call(
        by_row_kernel,
        out_shape=jax.ShapeDtypeStruct((COLS, P2_ROWS, BLK), jnp.float32),
        scratch_shapes=[pltpu.VMEM((LEV * TILES, BLK), jnp.float32)],
        compiler_params=pltpu.CompilerParams(vmem_limit_bytes=12 << 20),
        cost_estimate=pl.CostEstimate(flops=1_000_000, bytes_accessed=1_500_000, transcendentals=0),
        interpret=interpret,
        name="by_row",
    )(own, core, chip)


def stack_k(x):
    hi, lo = split2(x)
    return jnp.concatenate([hi, lo, hi], axis=0)


def filter_kernel(x_ref, f_ref, ft_ref, g_ref, gt_ref, tc_ref, ts_ref, gain_ref, out_ref):
    order = [p * 2 * LEV + h * LEV + l for p in range(2) for l in range(LEV) for h in range(2)]
    x = jnp.concatenate([x_ref[pl.ds(at, COLS, stride=P2_ROWS), :] for at in order], axis=1)
    tc, ts = tc_ref[...], ts_ref[...]
    y = dot32(f_ref[...], stack_k(x))
    rows = []
    for r in range(2 * LEV):
        re, im = y[:COLS, r * 256 : r * 256 + 256], y[COLS:, r * 256 : r * 256 + 256]
        rows.append(jnp.concatenate([re * tc + im * ts, im * tc - re * ts], axis=1))
    hi, lo = split2(jnp.concatenate(rows, axis=0))
    z = dot32(jnp.concatenate([hi, lo, hi], axis=1), g_ref[...]) * gain_ref[...]
    hi, lo = split2(z)
    middle = lax.broadcasted_iota(jnp.int32, z.shape, 1) // COLS == 1
    w = dot32(jnp.where(middle, lo.astype(jnp.float32), hi.astype(jnp.float32)).astype(jnp.bfloat16), gt_ref[...])
    cols = []
    for r in range(2 * LEV):
        part = w[r * COLS : r * COLS + COLS]
        re, im = part[:, :256], part[:, 256:]
        cols.append(jnp.concatenate([re * tc - im * ts, re * ts + im * tc], axis=0))
    out = dot32(ft_ref[...], stack_k(jnp.concatenate(cols, axis=1)))
    for i, at in enumerate(order):
        out_ref[pl.ds(at, COLS, stride=P2_ROWS), :] = out[:, i * BLK : i * BLK + BLK]


def zonal_filter(rows, tables, interpret=False):
    out = pl.pallas_call(
        filter_kernel,
        out_shape=jax.ShapeDtypeStruct((COLS * P2_ROWS, BLK), jnp.float32),
        compiler_params=pltpu.CompilerParams(vmem_limit_bytes=24 << 20),
        cost_estimate=pl.CostEstimate(flops=300_000_000, bytes_accessed=1_000_000, transcendentals=0),
        interpret=interpret,
        name="zonal",
    )(rows.reshape(COLS * P2_ROWS, BLK), *tables)
    return out.reshape(COLS, P2_ROWS, BLK)


def angles(zero, shape, factor, period):
    a = zero + lax.broadcasted_iota(jnp.int32, shape, 0)
    b = lax.broadcasted_iota(jnp.int32, shape, 1)
    phases = a * b * factor % period
    return phases.astype(jnp.float32) * (TWO_PI / period)


def three(x, axis):
    hi = lax.reduce_precision(x, 8, 7)
    return jnp.concatenate([hi, hi, x - hi], axis=axis).astype(jnp.bfloat16)


def zonal_tables(cutoff, zero):
    theta = angles(zero, (COLS, COLS), 1, COLS)
    f = jnp.concatenate([jnp.cos(theta), -jnp.sin(theta)], axis=0)
    turn = angles(zero, (COLS, 256), 1, NLON)
    tc, ts = jnp.cos(turn), jnp.sin(turn)
    phi = angles(zero, (KW // COLS, 256), COLS, NLON)
    inside = zero + lax.broadcasted_iota(jnp.int32, phi.shape, 1) < LON
    c, s = jnp.where(inside, jnp.cos(phi), 0.0), jnp.where(inside, jnp.sin(phi), 0.0)
    gt = jnp.concatenate([jnp.concatenate([c, s], axis=1), jnp.concatenate([-s, c], axis=1)], axis=0)
    g = jnp.concatenate([three(gt.T, 0)] * 3, axis=1)
    shape = (2, LEV, COLS, 3, 2, KW // COLS)
    k = zero + lax.broadcasted_iota(jnp.int32, shape, 2) + COLS * (zero + lax.broadcasted_iota(jnp.int32, shape, 5))
    gain = jnp.where(k == 0, 1.0, 2.0) / NLON
    gain = jnp.where(k <= cutoff.reshape(2, 1, 1, 1, 1, 1), gain, 0.0).reshape(2 * LEV * COLS, 3 * COLS)
    return three(f, 1), three(f.T, 1), g, three(gt, 0), tc, ts, gain


def lay_kernel(rows_ref, out_ref, low, high):
    for h, half in enumerate((low, high)):
        for p in range(2):
            for l in range(LEV):
                part = rows_ref[pl.ds(p * 2 * LEV + h * LEV + l, COLS, stride=P2_ROWS), :]
                half[pl.ds(l * LATB + p, COLS, stride=2), :] = part
    for l in range(LEV):
        out_ref[l, :, :BLK] = low[l * LATB : l * LATB + LATB, :]
        out_ref[l, :, BLK:] = high[l * LATB : l * LATB + LATB, : LON - BLK]


def by_latitude(rows, interpret=False):
    return pl.pallas_call(
        lay_kernel,
        out_shape=jax.ShapeDtypeStruct((LEV, LATB, LON), jnp.float32),
        scratch_shapes=[pltpu.VMEM((LEV * LATB, BLK), jnp.float32)] * 2,
        cost_estimate=pl.CostEstimate(flops=1_000_000, bytes_accessed=800_000, transcendentals=0),
        compiler_params=pltpu.CompilerParams(vmem_limit_bytes=8 << 20),
        interpret=interpret,
        name="lay",
    )(rows.reshape(COLS * P2_ROWS, BLK))


def exchange(array):
    return lax.all_to_all(array, "col", 0, 0, tiled=True)


def local(source, weights, source_block, owner_device, target_tile, cutoff):
    bands = lax.axis_size("band")
    got = exchange(place(source, weights, source_block, owner_device[:, 0], target_tile))
    got, cutoff, zero = lax.optimization_barrier((got.reshape(COLS * ROWS, BLK), cutoff, jnp.int32(0)))
    to_chip, to_core = tile_sums(got, (2, 0))
    pairs = [(i, i + 1 if i % 2 else i - 1) for i in range(1, bands - 1)]
    chip = lax.ppermute(to_chip, "band", pairs)
    core = lax.ppermute(to_core, "band", [(i, i ^ 1) for i in range(bands)])
    (own,) = tile_sums(got, (1,))
    rows = by_row(own, core, chip)
    remapped = by_latitude(rows)
    rows, remapped = lax.optimization_barrier((exchange(rows), remapped))
    rows = zonal_filter(rows, zonal_tables(cutoff, zero))
    filtered = by_latitude(exchange(rows))
    return (remapped, filtered)


def solution(mesh):
    in_specs = (
        P(None, ("band", "col")),
        P(("band", "col"), None, None),
        P(("band", "col")),
        P(("band", "col"), None),
        P(("band", "col")),
        P(("band", "col")),
    )
    out_specs = (P(None, "band", "col"), P(None, "band", "col"))
    return jax.shard_map(local, mesh=mesh, in_specs=in_specs, out_specs=out_specs, check_vma=False)
```

```python
import jax
import jax.numpy as jnp
from jax import lax
from jax.experimental import pallas as pl
from jax.experimental.pallas import tpu as pltpu
from jax.sharding import PartitionSpec as P

NLON = 7200
KW = 512
TWO_PI = 6.283185307179586

LEV = 6
BLK = 128
COLS = 32
LON = NLON // COLS
LATB = 64
CAP = 6
SIDE_ROWS = CAP * LEV
ID_ROW = 3 * SIDE_ROWS
ROWS = ID_ROW + 4
WINDOW = 8
TILES = 120
P2_ROWS = 24
CHUNK = 128
CHUNKS = 2
AXES = True


def split2(x):
    hi = x.astype(jnp.bfloat16)
    lo = (x - hi.astype(jnp.float32)).astype(jnp.bfloat16)
    return hi, lo


def dot32(a, b):
    return jnp.dot(a, b, preferred_element_type=jnp.float32)


def place_kernel(sb_hbm, owner_hbm, tile_hbm, src_hbm, w_hbm, buf, w, src, sb, owners, tiles, marks, count, w_sem, in_sem):
    def chunk_copy(i):
        part = pl.ds(i * CHUNK, CHUNK)
        return pltpu.make_async_copy(w_hbm.at[part], w.at[part], w_sem.at[i])

    small = [
        pltpu.make_async_copy(owner_hbm, owners, in_sem.at[0]),
        pltpu.make_async_copy(sb_hbm, sb, in_sem.at[1]),
        pltpu.make_async_copy(tile_hbm, tiles, in_sem.at[2]),
        pltpu.make_async_copy(src_hbm, src, in_sem.at[3]),
    ]
    for copy in small:
        copy.start()
    for i in range(CHUNKS):
        chunk_copy(i).start()
    for i in range(3 * COLS):
        count[i] = 0
    buf[...] = jnp.zeros_like(buf)
    marks[...] = jnp.zeros_like(marks)
    for copy in small:
        copy.wait()
    band = lax.axis_index("band").astype(jnp.int32) if AXES else 3
    col = lax.axis_index("col").astype(jnp.int32) if AXES else 5
    first = (band - 1) * COLS
    odd = band % 2
    side_base = jnp.where(odd == 1, 0, 2 * SIDE_ROWS)
    side_step = jnp.where(odd == 1, SIDE_ROWS, -SIDE_ROWS)
    lane = (lax.broadcasted_iota(jnp.int32, (1, BLK), 1) - col % (COLS // 2) * WINDOW) * LEV

    def chunk(i, carry):
        chunk_copy(i).wait()
        for u in range(CHUNK):
            n = i * CHUNK + u
            key = owners[n] - first
            start = pl.multiple_of(sb[n] * BLK, BLK)
            value = dot32(src[:, pl.ds(start, BLK)], w[n])
            row = count[key]
            count[key] = row + LEV
            buf[key & (COLS - 1), pl.ds((key >> 5) * side_step + (side_base + row), LEV), :] = value
            mark = jnp.where(lane == row, tiles[n] + 1, 0)
            marks[pl.ds(key, 1), :] = marks[pl.ds(key, 1), :] + mark.astype(jnp.float32)
        return carry

    lax.fori_loop(0, CHUNKS, chunk, 0)
    below, above = marks[:COLS, :], marks[2 * COLS :, :]
    marks[:COLS, :] = jnp.where(odd == 1, below, above)
    marks[2 * COLS :, :] = pltpu.roll(jnp.where(odd == 1, above, below), WINDOW - CAP, 1)
    for key in range(3 * COLS):
        row = ID_ROW + key // COLS
        buf[key % COLS, row : row + 1, :] = marks[key : key + 1, :]


def place(source, weights, source_block, owners, target_tile, interpret=False):
    hbm = pl.BlockSpec(memory_space=pltpu.HBM)
    blocks = weights.shape[0]
    return pl.pallas_call(
        place_kernel,
        out_shape=pltpu.VMEM((COLS, ROWS, BLK), jnp.float32),
        in_specs=[hbm] * 5,
        out_specs=pl.BlockSpec(memory_space=pltpu.VMEM),
        scratch_shapes=[
            pltpu.VMEM(weights.shape, weights.dtype),
            pltpu.VMEM(source.shape, source.dtype),
            pltpu.SMEM((blocks,), jnp.int32),
            pltpu.SMEM((blocks,), jnp.int32),
            pltpu.SMEM((blocks,), jnp.int32),
            pltpu.VMEM((3 * COLS, BLK), jnp.float32),
            pltpu.SMEM((3 * COLS,), jnp.int32),
            pltpu.SemaphoreType.DMA((CHUNKS,)),
            pltpu.SemaphoreType.DMA((4,)),
        ],
        compiler_params=pltpu.CompilerParams(vmem_limit_bytes=58 << 20),
        cost_estimate=pl.CostEstimate(flops=100_000_000, bytes_accessed=10_000_000, transcendentals=0),
        interpret=interpret,
        name="place",
    )(source_block, owners, target_tile, source, weights)


def sum_side(side, got_ref, out_ref):
    begin = min(side * CAP, 3 * CAP - WINDOW) * LEV
    halves = []
    for half in range(2):
        at = half * (COLS // 2) * ROWS + ID_ROW + side
        marks = [got_ref[pl.ds(at + g * 8 * ROWS, 8, stride=ROWS), :] for g in range(2)]
        halves.append(jnp.sum(marks[0] + marks[1], axis=0, keepdims=True))
    ids = jnp.concatenate(halves, axis=1)
    tile = lax.broadcasted_iota(jnp.int32, (TILES, 2 * BLK), 0).astype(jnp.float32) + 1.0
    chooser = jnp.where(tile == ids, 1.0, 0.0).astype(jnp.bfloat16)
    for l in range(LEV):
        data = [got_ref[pl.ds(s * ROWS + begin + l, WINDOW, stride=LEV), :] for s in range(COLS)]
        both = dot32(chooser, jnp.concatenate(split2(jnp.concatenate(data, axis=0)), axis=1))
        out_ref[l * TILES : l * TILES + TILES, :] = both[:, :BLK] + both[:, BLK:]


def tile_sums(got, sides, interpret=False):
    def kernel(got_ref, *out_refs):
        for side, out_ref in zip(sides, out_refs):
            sum_side(side, got_ref, out_ref)

    return pl.pallas_call(
        kernel,
        out_shape=[jax.ShapeDtypeStruct((LEV * TILES, BLK), jnp.float32)] * len(sides),
        compiler_params=pltpu.CompilerParams(vmem_limit_bytes=24 << 20),
        cost_estimate=pl.CostEstimate(flops=100_000_000 * len(sides), bytes_accessed=1_000_000, transcendentals=0),
        interpret=interpret,
    )(got)


def by_row_kernel(own_ref, core_ref, chip_ref, out_ref, sums):
    sums[...] = own_ref[...] + core_ref[...] + chip_ref[...]
    lane = lax.broadcasted_iota(jnp.int32, (LEV, BLK), 1)
    for lat in range(LATB):
        for half in range(2):
            first, shift = divmod(lat * LON + half * BLK, BLK)
            value = sums[pl.ds(first, LEV, stride=TILES), :]
            if shift:
                later = sums[pl.ds(first + 1, LEV, stride=TILES), :]
                value = jnp.where(lane < BLK - shift, pltpu.roll(value, BLK - shift, 1), pltpu.roll(later, BLK - shift, 1))
            at = (lat % 2) * 2 * LEV + half * LEV
            out_ref[lat // 2, at : at + LEV, :] = value


def by_row(own, core, chip, interpret=False):
    return pl.pallas_call(
        by_row_kernel,
        out_shape=jax.ShapeDtypeStruct((COLS, P2_ROWS, BLK), jnp.float32),
        scratch_shapes=[pltpu.VMEM((LEV * TILES, BLK), jnp.float32)],
        compiler_params=pltpu.CompilerParams(vmem_limit_bytes=12 << 20),
        cost_estimate=pl.CostEstimate(flops=1_000_000, bytes_accessed=1_500_000, transcendentals=0),
        interpret=interpret,
        name="by_row",
    )(own, core, chip)


def stack_k(x):
    hi, lo = split2(x)
    return jnp.concatenate([hi, lo, hi], axis=0)


def filter_kernel(x_ref, f_ref, ft_ref, g_ref, gt_ref, tc_ref, ts_ref, gain_ref, out_ref):
    order = [p * 2 * LEV + h * LEV + l for p in range(2) for l in range(LEV) for h in range(2)]
    x = jnp.concatenate([x_ref[pl.ds(at, COLS, stride=P2_ROWS), :] for at in order], axis=1)
    tc, ts = tc_ref[...], ts_ref[...]
    y = dot32(f_ref[...], stack_k(x))
    rows = []
    for r in range(2 * LEV):
        re, im = y[:COLS, r * 256 : r * 256 + 256], y[COLS:, r * 256 : r * 256 + 256]
        rows.append(jnp.concatenate([re * tc + im * ts, im * tc - re * ts], axis=1))
    hi, lo = split2(jnp.concatenate(rows, axis=0))
    z = dot32(jnp.concatenate([hi, lo, hi], axis=1), g_ref[...]) * gain_ref[...]
    hi, lo = split2(z)
    middle = lax.broadcasted_iota(jnp.int32, z.shape, 1) // COLS == 1
    w = dot32(jnp.where(middle, lo.astype(jnp.float32), hi.astype(jnp.float32)).astype(jnp.bfloat16), gt_ref[...])
    cols = []
    for r in range(2 * LEV):
        part = w[r * COLS : r * COLS + COLS]
        re, im = part[:, :256], part[:, 256:]
        cols.append(jnp.concatenate([re * tc - im * ts, re * ts + im * tc], axis=0))
    out = dot32(ft_ref[...], stack_k(jnp.concatenate(cols, axis=1)))
    for i, at in enumerate(order):
        out_ref[pl.ds(at, COLS, stride=P2_ROWS), :] = out[:, i * BLK : i * BLK + BLK]


def zonal_filter(rows, tables, interpret=False):
    out = pl.pallas_call(
        filter_kernel,
        out_shape=jax.ShapeDtypeStruct((COLS * P2_ROWS, BLK), jnp.float32),
        compiler_params=pltpu.CompilerParams(vmem_limit_bytes=24 << 20),
        cost_estimate=pl.CostEstimate(flops=300_000_000, bytes_accessed=1_000_000, transcendentals=0),
        interpret=interpret,
        name="zonal",
    )(rows.reshape(COLS * P2_ROWS, BLK), *tables)
    return out.reshape(COLS, P2_ROWS, BLK)


def angles(zero, shape, factor, period):
    a = zero + lax.broadcasted_iota(jnp.int32, shape, 0)
    b = lax.broadcasted_iota(jnp.int32, shape, 1)
    phases = a * b * factor % period
    return phases.astype(jnp.float32) * (TWO_PI / period)


def three(x, axis):
    hi = lax.reduce_precision(x, 8, 7)
    return jnp.concatenate([hi, hi, x - hi], axis=axis).astype(jnp.bfloat16)


def zonal_tables(cutoff, zero):
    theta = angles(zero, (COLS, COLS), 1, COLS)
    f = jnp.concatenate([jnp.cos(theta), -jnp.sin(theta)], axis=0)
    turn = angles(zero, (COLS, 256), 1, NLON)
    tc, ts = jnp.cos(turn), jnp.sin(turn)
    phi = angles(zero, (KW // COLS, 256), COLS, NLON)
    inside = zero + lax.broadcasted_iota(jnp.int32, phi.shape, 1) < LON
    c, s = jnp.where(inside, jnp.cos(phi), 0.0), jnp.where(inside, jnp.sin(phi), 0.0)
    gt = jnp.concatenate([jnp.concatenate([c, s], axis=1), jnp.concatenate([-s, c], axis=1)], axis=0)
    g = jnp.concatenate([three(gt.T, 0)] * 3, axis=1)
    shape = (2, LEV, COLS, 3, 2, KW // COLS)
    k = zero + lax.broadcasted_iota(jnp.int32, shape, 2) + COLS * (zero + lax.broadcasted_iota(jnp.int32, shape, 5))
    gain = jnp.where(k == 0, 1.0, 2.0) / NLON
    gain = jnp.where(k <= cutoff.reshape(2, 1, 1, 1, 1, 1), gain, 0.0).reshape(2 * LEV * COLS, 3 * COLS)
    return three(f, 1), three(f.T, 1), g, three(gt, 0), tc, ts, gain


def lay_kernel(rows_ref, out_ref, low, high):
    for h, half in enumerate((low, high)):
        for p in range(2):
            for l in range(LEV):
                part = rows_ref[pl.ds(p * 2 * LEV + h * LEV + l, COLS, stride=P2_ROWS), :]
                half[pl.ds(l * LATB + p, COLS, stride=2), :] = part
    for l in range(LEV):
        out_ref[l, :, :BLK] = low[l * LATB : l * LATB + LATB, :]
        out_ref[l, :, BLK:] = high[l * LATB : l * LATB + LATB, : LON - BLK]


def by_latitude(rows, interpret=False):
    return pl.pallas_call(
        lay_kernel,
        out_shape=jax.ShapeDtypeStruct((LEV, LATB, LON), jnp.float32),
        scratch_shapes=[pltpu.VMEM((LEV * LATB, BLK), jnp.float32)] * 2,
        cost_estimate=pl.CostEstimate(flops=1_000_000, bytes_accessed=800_000, transcendentals=0),
        compiler_params=pltpu.CompilerParams(vmem_limit_bytes=8 << 20),
        interpret=interpret,
        name="lay",
    )(rows.reshape(COLS * P2_ROWS, BLK))


def exchange(array):
    return lax.all_to_all(array, "col", 0, 0, tiled=True)


def local(source, weights, source_block, owner_device, target_tile, cutoff):
    bands = lax.axis_size("band")
    got = exchange(place(source, weights, source_block, owner_device[:, 0], target_tile))
    got = got.reshape(COLS * ROWS, BLK)
    to_chip, to_core = tile_sums(got, (2, 0))
    to_chip, to_core, cutoff, zero = lax.optimization_barrier((to_chip, to_core, cutoff, jnp.int32(0)))
    pairs = [(i, i + 1 if i % 2 else i - 1) for i in range(1, bands - 1)]
    chip = lax.ppermute(to_chip, "band", pairs)
    core = lax.ppermute(to_core, "band", [(i, i ^ 1) for i in range(bands)])
    (own,) = tile_sums(got, (1,))
    tables = zonal_tables(cutoff, zero)
    own, *tables = lax.optimization_barrier((own, *tables))
    rows = by_row(own, core, chip)
    remapped = by_latitude(rows)
    rows, remapped = lax.optimization_barrier((exchange(rows), remapped))
    rows = zonal_filter(rows, tables)
    filtered = by_latitude(exchange(rows))
    return (remapped, filtered)


def solution(mesh):
    in_specs = (
        P(None, ("band", "col")),
        P(("band", "col"), None, None),
        P(("band", "col")),
        P(("band", "col"), None),
        P(("band", "col")),
        P(("band", "col")),
    )
    out_specs = (P(None, "band", "col"), P(None, "band", "col"))
    return jax.shard_map(local, mesh=mesh, in_specs=in_specs, out_specs=out_specs, check_vma=False)
```

```python
import jax
import jax.numpy as jnp
from jax import lax
from jax.experimental import pallas as pl
from jax.experimental.pallas import tpu as pltpu
from jax.sharding import PartitionSpec as P

NLON = 7200
KW = 512
TWO_PI = 6.283185307179586

LEV = 6
BLK = 128
COLS = 32
LON = NLON // COLS
LATB = 64
CAP = 6
SIDE_ROWS = CAP * LEV
ID_ROW = 3 * SIDE_ROWS
ROWS = ID_ROW + 4
WINDOW = 8
TILES = 120
P2_ROWS = 24
PART = 8
CHUNK = 128
CHUNKS = 2
AXES = True


def split2(x):
    hi = x.astype(jnp.bfloat16)
    lo = (x - hi.astype(jnp.float32)).astype(jnp.bfloat16)
    return hi, lo


def dot32(a, b):
    return jnp.dot(a, b, preferred_element_type=jnp.float32)


def place_kernel(sb_hbm, owner_hbm, tile_hbm, src_hbm, w_hbm, buf, w, src, sb, owners, tiles, marks, count, w_sem, in_sem):
    def chunk_copy(i):
        part = pl.ds(i * CHUNK, CHUNK)
        return pltpu.make_async_copy(w_hbm.at[part], w.at[part], w_sem.at[i])

    small = [
        pltpu.make_async_copy(owner_hbm, owners, in_sem.at[0]),
        pltpu.make_async_copy(sb_hbm, sb, in_sem.at[1]),
        pltpu.make_async_copy(tile_hbm, tiles, in_sem.at[2]),
        pltpu.make_async_copy(src_hbm, src, in_sem.at[3]),
    ]
    for copy in small:
        copy.start()
    for i in range(CHUNKS):
        chunk_copy(i).start()
    for i in range(3 * COLS):
        count[i] = 0
    buf[...] = jnp.zeros_like(buf)
    marks[...] = jnp.zeros_like(marks)
    for copy in small:
        copy.wait()
    band = lax.axis_index("band").astype(jnp.int32) if AXES else 3
    col = lax.axis_index("col").astype(jnp.int32) if AXES else 5
    first = (band - 1) * COLS
    odd = band % 2
    side_base = jnp.where(odd == 1, 0, 2 * SIDE_ROWS)
    side_step = jnp.where(odd == 1, SIDE_ROWS, -SIDE_ROWS)
    lane = (lax.broadcasted_iota(jnp.int32, (1, BLK), 1) - col % (COLS // 2) * WINDOW) * LEV

    def chunk(i, carry):
        chunk_copy(i).wait()
        for u in range(CHUNK):
            n = i * CHUNK + u
            key = owners[n] - first
            start = pl.multiple_of(sb[n] * BLK, BLK)
            value = dot32(src[:, pl.ds(start, BLK)], w[n])
            row = count[key]
            count[key] = row + LEV
            buf[key & (COLS - 1), pl.ds((key >> 5) * side_step + (side_base + row), LEV), :] = value
            mark = jnp.where(lane == row, tiles[n] + 1, 0)
            marks[pl.ds(key, 1), :] = marks[pl.ds(key, 1), :] + mark.astype(jnp.float32)
        return carry

    lax.fori_loop(0, CHUNKS, chunk, 0)
    below, above = marks[:COLS, :], marks[2 * COLS :, :]
    marks[:COLS, :] = jnp.where(odd == 1, below, above)
    marks[2 * COLS :, :] = pltpu.roll(jnp.where(odd == 1, above, below), WINDOW - CAP, 1)
    for key in range(3 * COLS):
        row = ID_ROW + key // COLS
        buf[key % COLS, row : row + 1, :] = marks[key : key + 1, :]


def place(source, weights, source_block, owners, target_tile, interpret=False):
    hbm = pl.BlockSpec(memory_space=pltpu.HBM)
    blocks = weights.shape[0]
    return pl.pallas_call(
        place_kernel,
        out_shape=pltpu.VMEM((COLS, ROWS, BLK), jnp.float32),
        in_specs=[hbm] * 5,
        out_specs=pl.BlockSpec(memory_space=pltpu.VMEM),
        scratch_shapes=[
            pltpu.VMEM(weights.shape, weights.dtype),
            pltpu.VMEM(source.shape, source.dtype),
            pltpu.SMEM((blocks,), jnp.int32),
            pltpu.SMEM((blocks,), jnp.int32),
            pltpu.SMEM((blocks,), jnp.int32),
            pltpu.VMEM((3 * COLS, BLK), jnp.float32),
            pltpu.SMEM((3 * COLS,), jnp.int32),
            pltpu.SemaphoreType.DMA((CHUNKS,)),
            pltpu.SemaphoreType.DMA((4,)),
        ],
        compiler_params=pltpu.CompilerParams(vmem_limit_bytes=58 << 20),
        cost_estimate=pl.CostEstimate(flops=100_000_000, bytes_accessed=10_000_000, transcendentals=0),
        interpret=interpret,
        name="place",
    )(source_block, owners, target_tile, source, weights)


def sum_side(side, got_ref, out_ref):
    begin = min(side * CAP, 3 * CAP - WINDOW) * LEV
    halves = []
    for half in range(2):
        at = half * (COLS // 2) * ROWS + ID_ROW + side
        marks = [got_ref[pl.ds(at + g * 8 * ROWS, 8, stride=ROWS), :] for g in range(2)]
        halves.append(jnp.sum(marks[0] + marks[1], axis=0, keepdims=True))
    ids = jnp.concatenate(halves, axis=1)
    tile = lax.broadcasted_iota(jnp.int32, (TILES, 2 * BLK), 0).astype(jnp.float32) + 1.0
    chooser = jnp.where(tile == ids, 1.0, 0.0).astype(jnp.bfloat16)
    for l in range(LEV):
        data = [got_ref[pl.ds(s * ROWS + begin + l, WINDOW, stride=LEV), :] for s in range(COLS)]
        both = dot32(chooser, jnp.concatenate(split2(jnp.concatenate(data, axis=0)), axis=1))
        out_ref[l * TILES : l * TILES + TILES, :] = both[:, :BLK] + both[:, BLK:]


def tile_sums(got, sides, interpret=False):
    def kernel(got_ref, *out_refs):
        for side, out_ref in zip(sides, out_refs):
            sum_side(side, got_ref, out_ref)

    return pl.pallas_call(
        kernel,
        out_shape=[jax.ShapeDtypeStruct((LEV * TILES, BLK), jnp.float32)] * len(sides),
        compiler_params=pltpu.CompilerParams(vmem_limit_bytes=24 << 20),
        cost_estimate=pl.CostEstimate(flops=100_000_000 * len(sides), bytes_accessed=1_000_000, transcendentals=0),
        interpret=interpret,
    )(got)


def by_row_kernel(own_ref, core_ref, chip_ref, out_hbm, sums, out_ref, sem):
    def part_copy(i):
        part = pl.ds(i * PART, PART)
        return pltpu.make_async_copy(out_ref.at[part], out_hbm.at[part], sem.at[i])

    sums[...] = own_ref[...] + core_ref[...] + chip_ref[...]
    lane = lax.broadcasted_iota(jnp.int32, (LEV, BLK), 1)
    for lat in range(LATB):
        for half in range(2):
            first, shift = divmod(lat * LON + half * BLK, BLK)
            value = sums[pl.ds(first, LEV, stride=TILES), :]
            if shift:
                later = sums[pl.ds(first + 1, LEV, stride=TILES), :]
                value = jnp.where(lane < BLK - shift, pltpu.roll(value, BLK - shift, 1), pltpu.roll(later, BLK - shift, 1))
            at = (lat % 2) * 2 * LEV + half * LEV
            out_ref[lat // 2, at : at + LEV, :] = value
        if (lat + 1) % (2 * PART) == 0:
            part_copy(lat // (2 * PART)).start()
    for i in range(COLS // PART):
        part_copy(i).wait()


def by_row(own, core, chip, interpret=False):
    return pl.pallas_call(
        by_row_kernel,
        out_shape=jax.ShapeDtypeStruct((COLS, P2_ROWS, BLK), jnp.float32),
        out_specs=pl.BlockSpec(memory_space=pltpu.HBM),
        scratch_shapes=[
            pltpu.VMEM((LEV * TILES, BLK), jnp.float32),
            pltpu.VMEM((COLS, P2_ROWS, BLK), jnp.float32),
            pltpu.SemaphoreType.DMA((COLS // PART,)),
        ],
        compiler_params=pltpu.CompilerParams(vmem_limit_bytes=12 << 20),
        cost_estimate=pl.CostEstimate(flops=1_000_000, bytes_accessed=1_500_000, transcendentals=0),
        interpret=interpret,
        name="by_row",
    )(own, core, chip)


def stack_k(x):
    hi, lo = split2(x)
    return jnp.concatenate([hi, lo, hi], axis=0)


def filter_kernel(x_ref, f_ref, ft_ref, g_ref, gt_ref, tc_ref, ts_ref, gain_ref, out_ref):
    order = [p * 2 * LEV + h * LEV + l for p in range(2) for l in range(LEV) for h in range(2)]
    x = jnp.concatenate([x_ref[pl.ds(at, COLS, stride=P2_ROWS), :] for at in order], axis=1)
    tc, ts = tc_ref[...], ts_ref[...]
    y = dot32(f_ref[...], stack_k(x))
    rows = []
    for r in range(2 * LEV):
        re, im = y[:COLS, r * 256 : r * 256 + 256], y[COLS:, r * 256 : r * 256 + 256]
        rows.append(jnp.concatenate([re * tc + im * ts, im * tc - re * ts], axis=1))
    hi, lo = split2(jnp.concatenate(rows, axis=0))
    z = dot32(jnp.concatenate([hi, lo, hi], axis=1), g_ref[...]) * gain_ref[...]
    hi, lo = split2(z)
    middle = lax.broadcasted_iota(jnp.int32, z.shape, 1) // COLS == 1
    w = dot32(jnp.where(middle, lo.astype(jnp.float32), hi.astype(jnp.float32)).astype(jnp.bfloat16), gt_ref[...])
    cols = []
    for r in range(2 * LEV):
        part = w[r * COLS : r * COLS + COLS]
        re, im = part[:, :256], part[:, 256:]
        cols.append(jnp.concatenate([re * tc - im * ts, re * ts + im * tc], axis=0))
    out = dot32(ft_ref[...], stack_k(jnp.concatenate(cols, axis=1)))
    for i, at in enumerate(order):
        out_ref[pl.ds(at, COLS, stride=P2_ROWS), :] = out[:, i * BLK : i * BLK + BLK]


def zonal_filter(rows, tables, interpret=False):
    out = pl.pallas_call(
        filter_kernel,
        out_shape=jax.ShapeDtypeStruct((COLS * P2_ROWS, BLK), jnp.float32),
        compiler_params=pltpu.CompilerParams(vmem_limit_bytes=24 << 20),
        cost_estimate=pl.CostEstimate(flops=300_000_000, bytes_accessed=1_000_000, transcendentals=0),
        interpret=interpret,
        name="zonal",
    )(rows.reshape(COLS * P2_ROWS, BLK), *tables)
    return out.reshape(COLS, P2_ROWS, BLK)


def angles(zero, shape, factor, period):
    a = zero + lax.broadcasted_iota(jnp.int32, shape, 0)
    b = lax.broadcasted_iota(jnp.int32, shape, 1)
    phases = a * b * factor % period
    return phases.astype(jnp.float32) * (TWO_PI / period)


def three(x, axis):
    hi = lax.reduce_precision(x, 8, 7)
    return jnp.concatenate([hi, hi, x - hi], axis=axis).astype(jnp.bfloat16)


def zonal_tables(cutoff, zero):
    theta = angles(zero, (COLS, COLS), 1, COLS)
    f = jnp.concatenate([jnp.cos(theta), -jnp.sin(theta)], axis=0)
    turn = angles(zero, (COLS, 256), 1, NLON)
    tc, ts = jnp.cos(turn), jnp.sin(turn)
    phi = angles(zero, (KW // COLS, 256), COLS, NLON)
    inside = zero + lax.broadcasted_iota(jnp.int32, phi.shape, 1) < LON
    c, s = jnp.where(inside, jnp.cos(phi), 0.0), jnp.where(inside, jnp.sin(phi), 0.0)
    gt = jnp.concatenate([jnp.concatenate([c, s], axis=1), jnp.concatenate([-s, c], axis=1)], axis=0)
    g = jnp.concatenate([three(gt.T, 0)] * 3, axis=1)
    shape = (2, LEV, COLS, 3, 2, KW // COLS)
    k = zero + lax.broadcasted_iota(jnp.int32, shape, 2) + COLS * (zero + lax.broadcasted_iota(jnp.int32, shape, 5))
    gain = jnp.where(k == 0, 1.0, 2.0) / NLON
    gain = jnp.where(k <= cutoff.reshape(2, 1, 1, 1, 1, 1), gain, 0.0).reshape(2 * LEV * COLS, 3 * COLS)
    return three(f, 1), three(f.T, 1), g, three(gt, 0), tc, ts, gain


def lay_kernel(rows_ref, out_hbm, low, high, out_ref, sem):
    copies = [pltpu.make_async_copy(out_ref.at[l], out_hbm.at[l], sem.at[l]) for l in range(LEV)]
    for l in range(LEV):
        for h, half in enumerate((low, high)):
            for p in range(2):
                part = rows_ref[pl.ds(p * 2 * LEV + h * LEV + l, COLS, stride=P2_ROWS), :]
                half[pl.ds(l * LATB + p, COLS, stride=2), :] = part
        out_ref[l, :, :BLK] = low[l * LATB : l * LATB + LATB, :]
        out_ref[l, :, BLK:] = high[l * LATB : l * LATB + LATB, : LON - BLK]
        copies[l].start()
    for copy in copies:
        copy.wait()


def by_latitude(rows, interpret=False):
    return pl.pallas_call(
        lay_kernel,
        out_shape=jax.ShapeDtypeStruct((LEV, LATB, LON), jnp.float32),
        out_specs=pl.BlockSpec(memory_space=pltpu.HBM),
        scratch_shapes=[pltpu.VMEM((LEV * LATB, BLK), jnp.float32)] * 2
        + [pltpu.VMEM((LEV, LATB, LON), jnp.float32), pltpu.SemaphoreType.DMA((LEV,))],
        cost_estimate=pl.CostEstimate(flops=1_000_000, bytes_accessed=800_000, transcendentals=0),
        compiler_params=pltpu.CompilerParams(vmem_limit_bytes=8 << 20),
        interpret=interpret,
        name="lay",
    )(rows.reshape(COLS * P2_ROWS, BLK))


def exchange(array):
    return lax.all_to_all(array, "col", 0, 0, tiled=True)


def local(source, weights, source_block, owner_device, target_tile, cutoff):
    bands = lax.axis_size("band")
    got = exchange(place(source, weights, source_block, owner_device[:, 0], target_tile))
    got = got.reshape(COLS * ROWS, BLK)
    to_chip, to_core = tile_sums(got, (2, 0))
    to_chip, to_core, cutoff, zero = lax.optimization_barrier((to_chip, to_core, cutoff, jnp.int32(0)))
    pairs = [(i, i + 1 if i % 2 else i - 1) for i in range(1, bands - 1)]
    chip = lax.ppermute(to_chip, "band", pairs)
    core = lax.ppermute(to_core, "band", [(i, i ^ 1) for i in range(bands)])
    (own,) = tile_sums(got, (1,))
    tables = zonal_tables(cutoff, zero)
    own, *tables = lax.optimization_barrier((own, *tables))
    rows = by_row(own, core, chip)
    remapped = by_latitude(rows)
    rows, remapped = lax.optimization_barrier((exchange(rows), remapped))
    rows = zonal_filter(rows, tables)
    filtered = by_latitude(exchange(rows))
    return (remapped, filtered)


def solution(mesh):
    in_specs = (
        P(None, ("band", "col")),
        P(("band", "col"), None, None),
        P(("band", "col")),
        P(("band", "col"), None),
        P(("band", "col")),
        P(("band", "col")),
    )
    out_specs = (P(None, "band", "col"), P(None, "band", "col"))
    return jax.shard_map(local, mesh=mesh, in_specs=in_specs, out_specs=out_specs, check_vma=False)
```
